8 devices in a mesh: batch: 1 (over z), row: 2 (over y), col: 4 (over x, core).
Axes of the slice: x: 2, y: 2, z: 1, core: 2. Of those that a mesh axis runs over, the one named last changes fastest.
Arguments:
- l_mat: bfloat16 [14336, 14336], P(('batch', 'row'), 'col')
- b_mat: bfloat16 [14336, 8192], P(('batch', 'row'), 'col')
Outputs:
- output: bfloat16 [14336, 8192], P(('batch', 'row'), 'col')
All inputs are finite; a program needn't handle non-finite values.
Results may differ from the reference program's by a relative error of at most 0.001.
Values are sent between devices in bfloat16 or wider.
A program may use at most 1 GiB of HBM per device.

```python
import jax
import jax.numpy as jnp

N = 14336
M = 8192


def setup_inputs(seed: int = 0, part: int = 0) -> dict:
    base_key = jax.random.fold_in(jax.random.key(seed), part)
    key_l, key_b = jax.random.split(base_key)
    row_scale = 1.0 / jnp.sqrt(jnp.arange(N, dtype=jnp.float32) + 1.0)
    l_full = jax.random.normal(key_l, (N, N), jnp.float32)
    l_mat = jnp.tril(l_full) * row_scale[:, None]
    b_mat = jax.random.normal(key_b, (N, M), jnp.float32)
    return {'l_mat': l_mat.astype(jnp.bfloat16), 'b_mat': b_mat.astype(jnp.bfloat16)}


def reference(l_mat, b_mat):
    product = jnp.dot(l_mat, b_mat, preferred_element_type=jnp.float32)
    return product.astype(jnp.bfloat16)
```

```python
import functools

import jax
import jax.numpy as jnp
from jax import lax
from jax.experimental import pallas as pl
from jax.experimental.pallas import tpu as pltpu
from jax.sharding import PartitionSpec as P

MESH = pl.DeviceIdType.MESH
S = 896
KT = 1792
NT = 1024
UNIT = 224
RELAY = 25


def kernel(l_ref, b_ref, x_ref, lap, lbr, lbp, brem, lt, bt, acc, ot,
           lsem, bsem, osem, zsem, gsem, bs, br, ls, lr, ps, pr, qs, qr):
    batch, row, col = lax.axis_index('batch'), lax.axis_index('row'), lax.axis_index('col')
    x, c = col // 2, col % 2
    is_a = (row == 0) & (x == 0)
    is_b = (row == 0) & (x == 1)
    is_c = (row == 1) & (x == 0)
    is_d = (row == 1) & (x == 1)
    half = l_ref.shape[1]
    peer = (batch, row, 2 * x + 1 - c)
    across = (batch, row, 2 * (1 - x) + c)
    along = (batch, 1 - row, col)
    diag = (batch, 1 - row, 2 * (1 - x) + c)

    barrier = pltpu.get_barrier_semaphore()
    for device in (peer, across, along, diag):
        pl.semaphore_signal(barrier, inc=1, device_id=device, device_id_type=MESH)
    pl.semaphore_wait(barrier, 4)

    def remote(src, dst, send, recv, device):
        return pltpu.make_async_remote_copy(
            src_ref=src, dst_ref=dst, send_sem=send, recv_sem=recv,
            device_id=device, device_id_type=MESH)

    def b_copy(n):
        cols = pl.ds(n * NT, NT)
        return remote(b_ref.at[:, cols], brem.at[:, cols], bs.at[n], br.at[n], along)

    def tri_copy(i, h):
        width = min((i + 1) * S - h * half, half)
        rows, cols = pl.ds(i * S, S), pl.ds(0, width)
        return remote(l_ref.at[rows, cols], lbr.at[rows, cols], ls.at[i], lr.at[i], across)

    def full_copy(i):
        rows = pl.ds(i * S, S)
        return remote(l_ref.at[rows], lbr.at[rows], ls.at[i], lr.at[i], across)

    def unit_copy(u, src, device):
        rows = pl.ds(u * UNIT, UNIT)
        return remote(src.at[rows], lbr.at[rows], ls.at[u - 16], lr.at[u - 16], device)

    def la_copy(i):
        rows = pl.ds(i * S, S)
        return remote(l_ref.at[rows], lap.at[rows], ps.at[i], pr.at[i], peer)

    def lb_copy(i):
        rows = pl.ds(i * S, S)
        return remote(lbr.at[rows], lbp.at[rows], qs.at[i], qr.at[i], peer)

    tri_pairs = [(i, h) for h in (0, 1) for i in range(4 * h, 8)]

    def each_tri(do):
        for h in (0, 1):
            @pl.when(c == h)
            def _():
                for i in range(4 * h, 8):
                    do(i, h)

    def each_la(do):
        @pl.when(is_c | (c == 0))
        def _():
            for i in range(4):
                do(i)
        for i in range(4, 8):
            do(i)

    @pl.when(~is_b)
    def _():
        each_la(lambda i: la_copy(i).start())

    @pl.when(row == 0)
    def _():
        for n in range(2):
            b_copy(n).start()

    @pl.when(is_a | is_d)
    def _():
        each_tri(lambda i, h: tri_copy(i, h).start())

    @pl.when(is_c)
    def _():
        for u in list(range(28, 32)) + list(range(RELAY, 28)):
            unit_copy(u, l_ref, along).start()
        unit_copy(24, l_ref, across).start()
        for i in range(6):
            full_copy(i).start()

    @pl.when(is_b | is_c)
    def _():
        ot[0] = jnp.zeros_like(ot[0])
        corners = [
            pltpu.make_async_copy(
                ot.at[0, :, pl.ds(0, S)],
                lbr.at[pl.ds(pl.multiple_of((4 * c + j) * S, S), S), pl.ds((j + 1) * S, S)],
                zsem.at[j // 2])
            for j in (0, 2)]
        for copy in corners:
            copy.start()
        for copy in corners:
            copy.wait()

    def strip_of(r):
        q = r - 8
        i_d = jnp.where(r < 4, r, jnp.where(r < 8, r - 4, jnp.where(q < 2, 4, jnp.where(q < 4, 7, 3 + q // 2))))
        n_d = jnp.where(r < 4, 0, jnp.where(r < 8, 1, q % 2))
        return jnp.where(is_d, i_d, r % 8), jnp.where(is_d, n_d, r // 8)

    def counts(i):
        tri = i // 2 + 1
        na = jnp.where(is_c, 4, jnp.where(is_b, 0, tri))
        nb = jnp.where(is_d, 4, jnp.where(is_a, 0, tri))
        return na, nb

    def own_count(nk):
        first = jnp.minimum(nk, 2)
        return jnp.where(c == 0, first, nk - first)

    def arrive(i, nb_own):
        for k in range(8):
            @pl.when(i == k)
            def _():
                @pl.when(is_d)
                def _():
                    if k < 6:
                        full_copy(k).wait_recv()
                    else:
                        for u in range(4 * k, 4 * k + 4):
                            unit_copy(u, l_ref, across).wait_recv()

                @pl.when(~is_d)
                def _():
                    for h in (0, 1):
                        if k >= 4 * h:
                            @pl.when(c == h)
                            def _():
                                tri_copy(k, h).wait_recv()

                @pl.when(nb_own > 0)
                def _():
                    lb_copy(k).start()

    def fetch(r, t, slot):
        i, n = strip_of(r)
        na, nb = counts(i)
        in_a = t < na
        tt = jnp.where(in_a, t, t - na)
        nk = jnp.where(in_a, na, nb)
        own = own_count(nk)
        mine = tt < own
        kt = jnp.where(mine, 2 * c + tt, 2 * (1 - c) + tt - own)
        first = n == 0

        @pl.when(first & jnp.logical_not(in_a) & (tt == 0))
        def _():
            arrive(i, own)

        @pl.when(first & jnp.logical_not(mine) & (tt == own))
        def _():
            @pl.when(in_a)
            def _():
                la_copy(i).wait_recv()

            @pl.when(jnp.logical_not(in_a))
            def _():
                lb_copy(i).wait_recv()

        use_rem = (is_c & in_a) | (is_d & jnp.logical_not(in_a))

        @pl.when(use_rem & (i == 0) & (tt == 0))
        def _():
            b_copy(n).wait_recv()

        rows = pl.ds(pl.multiple_of(i * S, S), S)
        cols = pl.ds(pl.multiple_of((kt % 2) * KT, KT), KT)
        for pick, ref in (
            (in_a & mine, l_ref),
            (in_a & jnp.logical_not(mine), lap),
            (jnp.logical_not(in_a) & mine, lbr),
            (jnp.logical_not(in_a) & jnp.logical_not(mine), lbp),
        ):
            @pl.when(pick)
            def _():
                pltpu.make_async_copy(ref.at[rows, cols], lt.at[slot], lsem.at[slot]).start()
        depth = pl.ds(pl.multiple_of(kt * KT, KT), KT)
        ncols = pl.ds(pl.multiple_of(n * NT, NT), NT)
        for pick, ref in ((use_rem, brem), (jnp.logical_not(use_rem), b_ref)):
            @pl.when(pick)
            def _():
                pltpu.make_async_copy(ref.at[depth, ncols], bt.at[slot], bsem.at[slot]).start()

    def store(r, slot):
        i, n = strip_of(r)
        rows = pl.ds(pl.multiple_of(i * S, S), S)
        cols = pl.ds(pl.multiple_of(n * NT, NT), NT)
        return pltpu.make_async_copy(ot.at[slot], x_ref.at[rows, cols], osem.at[slot])

    steps = jnp.where(row == 0, 40, 104)
    fetch(jnp.int32(0), jnp.int32(0), 0)

    def step(s, state):
        r, t = state
        i, _ = strip_of(r)
        na, nb = counts(i)
        last = t + 1 == na + nb
        r_next = jnp.where(last, r + 1, r)
        t_next = jnp.where(last, 0, t + 1)
        slot = s % 2

        @pl.when(s + 1 < steps)
        def _():
            fetch(r_next, t_next, 1 - slot)

        @pl.when(t == 0)
        def _():
            acc[...] = jnp.zeros_like(acc)

        pltpu.make_async_copy(l_ref.at[pl.ds(0, S), pl.ds(0, KT)], lt.at[slot], lsem.at[slot]).wait()
        pltpu.make_async_copy(b_ref.at[pl.ds(0, KT), pl.ds(0, NT)], bt.at[slot], bsem.at[slot]).wait()
        acc[...] += jnp.dot(lt[slot], bt[slot], preferred_element_type=jnp.float32)

        @pl.when(last)
        def _():
            oslot = r % 2

            @pl.when(r >= 2)
            def _():
                store(r - 2, oslot).wait()
            ot[oslot] = acc[...].astype(ot.dtype)
            store(r, oslot).start()
        return r_next, t_next

    lax.fori_loop(0, steps, step, (jnp.int32(0), jnp.int32(0)))
    store(jnp.int32(14), 0).wait()
    store(jnp.int32(15), 1).wait()

    relayed = list(range(28, 32)) + list(range(RELAY, 28))

    @pl.when(is_a)
    def _():
        each_tri(lambda i, h: tri_copy(i, h).wait_send())
        for n in range(2):
            b_copy(n).wait_send()
        pl.semaphore_signal(gsem, inc=1, device_id=peer, device_id_type=MESH)
        pl.semaphore_wait(gsem, 1)
        for u in relayed:
            unit_copy(u, lbr, diag).wait_recv()
            unit_copy(u, lbr, diag).start()

    @pl.when(~is_b)
    def _():
        each_la(lambda i: la_copy(i).wait_send())

    @pl.when(is_b)
    def _():
        for n in range(2):
            b_copy(n).wait_send()

    @pl.when(is_d)
    def _():
        each_tri(lambda i, h: tri_copy(i, h).wait_send())

    @pl.when(is_c)
    def _():
        for i in range(6):
            full_copy(i).wait_send()
        unit_copy(24, l_ref, across).wait_send()

    @pl.when(is_c | is_a)
    def _():
        for u in range(RELAY, 32):
            unit_copy(u, l_ref, along).wait_send()

    @pl.when(~is_a)
    def _():
        @pl.when(is_d | (c == 0))
        def _():
            for i in range(4):
                lb_copy(i).wait_send()
        for i in range(4, 8):
            lb_copy(i).wait_send()


def solution(mesh):
    block_spec = P(('batch', 'row'), 'col')

    def local_product(l_block, b_block):
        rows, half = l_block.shape
        columns = b_block.shape[1]
        l_like = jax.ShapeDtypeStruct((rows, half), l_block.dtype)
        b_like = jax.ShapeDtypeStruct((rows, columns), b_block.dtype)
        dma = pltpu.SemaphoreType.DMA
        out = pl.pallas_call(
            kernel,
            out_shape=[b_like, l_like, l_like, l_like, b_like],
            in_specs=[pl.BlockSpec(memory_space=pl.ANY)] * 2,
            out_specs=[pl.BlockSpec(memory_space=pl.ANY)] * 5,
            scratch_shapes=[
                pltpu.VMEM((2, S, KT), l_block.dtype),
                pltpu.VMEM((2, KT, NT), b_block.dtype),
                pltpu.VMEM((S, NT), jnp.float32),
                pltpu.VMEM((2, S, NT), b_block.dtype),
                dma((2,)), dma((2,)), dma((2,)), dma((2,)), pltpu.SemaphoreType.REGULAR,
                dma((2,)), dma((2,)), dma((16,)), dma((16,)),
                dma((8,)), dma((8,)), dma((8,)), dma((8,)),
            ],
            compiler_params=pltpu.CompilerParams(
                collective_id=0, has_side_effects=True, vmem_limit_bytes=48 * 2**20),
            name='triangular_product',
        )(l_block, b_block)
        return out[0]

    return jax.shard_map(local_product, mesh=mesh, in_specs=(block_spec, block_spec),
                         out_specs=block_spec, check_vma=False)
```

```python
import jax
import jax.numpy as jnp
from jax import lax
from jax.experimental import pallas as pl
from jax.experimental.pallas import tpu as pltpu
from jax.sharding import PartitionSpec as P

MESH = pl.DeviceIdType.MESH
S = 896
KT = 1792
NT = 1024


def kernel(l_ref, b_ref, x_ref, lap, lbr, lbp, brem, xst, lt, bt, acc, ot,
           lsem, bsem, osem, zsem, bs, br, ls, lr, ps, pr, qs, qr, xs, xr):
    batch, row, col = lax.axis_index('batch'), lax.axis_index('row'), lax.axis_index('col')
    x, c = col // 2, col % 2
    is_a = (row == 0) & (x == 0)
    is_b = (row == 0) & (x == 1)
    is_c = (row == 1) & (x == 0)
    is_d = (row == 1) & (x == 1)
    half = l_ref.shape[1]
    peer = (batch, row, 2 * x + 1 - c)
    across = (batch, row, 2 * (1 - x) + c)
    along = (batch, 1 - row, col)

    barrier = pltpu.get_barrier_semaphore()
    for device in (peer, across, along):
        pl.semaphore_signal(barrier, inc=1, device_id=device, device_id_type=MESH)
    pl.semaphore_wait(barrier, 3)

    def remote(src, dst, send, recv, device):
        return pltpu.make_async_remote_copy(
            src_ref=src, dst_ref=dst, send_sem=send, recv_sem=recv,
            device_id=device, device_id_type=MESH)

    def strip(i, lo=0, width=None):
        return pl.ds(i * S, S), pl.ds(lo, half if width is None else width)

    def send_l(src, i, k, out, device, lo=0, width=None):
        return remote(src.at[strip(i, lo, width)], lbr.at[strip(k, lo, width)],
                      ls.at[out], lr.at[k if lo == 0 else 8], device)

    def tri_width(i, h):
        return min((i + 1) * S - h * half, half)

    def send_tri(i, h):
        return send_l(l_ref, i, i, i, across, 0, tri_width(i, h))

    def send_b(n, out, device):
        cols = pl.ds(n * NT, NT)
        return remote(b_ref.at[:, cols], brem.at[:, cols], bs.at[out], br.at[n], device)

    def send_b_top():
        rows = pl.ds(0, KT)
        return remote(b_ref.at[rows], brem.at[rows], bs.at[0], br.at[0], along)

    def send_c(i):
        if i < 2:
            return [send_l(l_ref, i, i, i, along)]
        if i < 7:
            return [send_l(l_ref, i, i, i, across)]
        return [send_l(l_ref, i, i, 7, across, 0, KT), send_l(l_ref, i, i, 8, across, KT, KT)]

    def relay(j):
        return send_l(lbr, j, 4 + j, 8 + j, across)

    def send_l11_top(j):
        return send_l(l_ref, j, 6 + j, 8 + j, along, 0, tri_width(j, 0))

    def la_copy(i):
        rows = pl.ds(i * S, S)
        return remote(l_ref.at[rows], lap.at[rows], ps.at[i], pr.at[i], peer)

    def lb_copy(i, lo=0, width=None):
        at = strip(i, lo, width)
        k = i if lo == 0 else 8
        return remote(lbr.at[at], lbp.at[at], qs.at[k], qr.at[k], peer)

    def send_x(i, n, k):
        cols = pl.ds(pl.multiple_of(n * NT, NT), NT)
        src = pl.ds(pl.multiple_of(i % 4 * S, S), S)
        dst = pl.ds(pl.multiple_of(i * S, S), S)
        target = (batch, jnp.where(is_a, row, 1 - row), jnp.where(is_a, 2 * (1 - x) + c, col))
        return remote(xst.at[src, cols], x_ref.at[dst, cols], xs.at[k], xr.at[k], target)

    def each_tri(do):
        for h in (0, 1):
            @pl.when(c == h)
            def _():
                for i in range(4 * h, 8):
                    do(i, h)

    def each_la(do):
        @pl.when(is_c | (is_a & (c == 0)))
        def _():
            for i in range(2):
                do(i)

        @pl.when(is_c | (c == 0))
        def _():
            for i in range(2, 4):
                do(i)
        for i in range(4, 8):
            do(i)

    def own_sends(do):
        @pl.when(is_a)
        def _():
            for n in range(2):
                do(send_b(n, n, along))

            @pl.when(c == 0)
            def _():
                for i in range(4):
                    do(send_tri(i, 0))

        @pl.when(is_b)
        def _():
            for n in range(2):
                do(send_b(n, n, along))
                do(send_b(n, 2 + n, across))

        @pl.when(is_c)
        def _():
            for i in range(8):
                for copy in send_c(i):
                    do(copy)

        @pl.when(is_d)
        def _():
            @pl.when(c == 0)
            def _():
                for j in range(2):
                    do(send_l11_top(j))
            do(send_b_top())
            each_tri(lambda i, h: do(send_tri(i, h)))

        @pl.when(jnp.logical_not(is_b))
        def _():
            each_la(lambda i: do(la_copy(i)))

    own_sends(lambda copy: copy.start())

    def zero_corner(k, j):
        @pl.when((is_c & (c == k // 4)) | (is_b & (c == 0) & (k != 4)))
        def _():
            cols = pl.ds((1 if k in (0, 4) or j == 6 else 3) * S, S)
            copy = pltpu.make_async_copy(ot.at[:, pl.ds(0, S)], lbr.at[pl.ds(k * S, S), cols], zsem)
            copy.start()
            copy.wait()

    @pl.when(is_b | is_c)
    def _():
        ot[...] = jnp.zeros_like(ot)
        for k in (0, 2, 4):
            zero_corner(k, k)

        @pl.when(is_c & (c == 1))
        def _():
            copy = pltpu.make_async_copy(
                ot.at[:, pl.ds(0, S)], lbr.at[pl.ds(6 * S, S), pl.ds(3 * S, S)], zsem)
            copy.start()
            copy.wait()

        @pl.when(is_b & (c == 0))
        def _():
            copy = pltpu.make_async_copy(
                ot.at[:, pl.ds(0, S)], lbr.at[pl.ds(6 * S, S), pl.ds(S, S)], zsem)
            copy.start()
            copy.wait()

    def pick(a, b, c_, d):
        return jnp.where(is_a, a, jnp.where(is_b, b, jnp.where(is_c, c_, d)))

    def run_of(r):
        late = pick(r >= 16, r >= 8, False, False)
        i = pick(jnp.where(late, 4 + r % 4, r % 8), jnp.where(late, r % 2, r % 4),
                 r % 8, jnp.where(r >= 8, r - 2, 2 + r % 4))
        n = pick(jnp.where(late, (r - 16) // 4, r // 8), jnp.where(late, (r - 8) // 2, r // 4),
                 r // 8, jnp.where(r >= 8, 0, r // 4))
        pair = is_d & (r >= 8)
        tri = i // 2 + 1
        na = pick(tri, 0, 4, tri)
        nb = pick(0, jnp.where(late, 4, tri), tri, 4)
        nc = jnp.where(is_b & late, 1, 0)
        return late, i, n, pair, na, nb, nc

    def place(n, pair, t):
        return jnp.where(pair, t % 2, n), jnp.where(pair, t // 2, t)

    def arrive(k_dyn, own):
        for k in range(8):
            @pl.when(k_dyn == k)
            def _():
                @pl.when(is_d)
                def _():
                    if k < 7:
                        send_l(l_ref, k, k, k, across).wait_recv()
                    else:
                        send_l(l_ref, k, k, k, across, 0, KT).wait_recv()

                @pl.when(is_c)
                def _():
                    for h in (0, 1):
                        if k >= 4 * h:
                            @pl.when(c == h)
                            def _():
                                send_tri(k, h).wait_recv()

                @pl.when(is_b)
                def _():
                    if k in (4, 5):
                        send_l(l_ref, k, k, k, across).wait_recv()
                    else:
                        @pl.when(c == 0)
                        def _():
                            send_l(l_ref, k, k, k, across, 0, tri_width(k % 6, 0)).wait_recv()

                @pl.when(own > 0)
                def _():
                    if k < 7:
                        lb_copy(k).start()
                    else:
                        @pl.when(is_d)
                        def _():
                            lb_copy(k, 0, KT).start()

                        @pl.when(jnp.logical_not(is_d))
                        def _():
                            lb_copy(k).start()

    def wait_peer(k_dyn):
        for k in range(8):
            @pl.when(k_dyn == k)
            def _():
                if k < 7:
                    lb_copy(k).wait_recv()
                else:
                    @pl.when(is_d)
                    def _():
                        lb_copy(k, 0, KT).wait_recv()

                    @pl.when(jnp.logical_not(is_d))
                    def _():
                        lb_copy(k).wait_recv()

    def fetch(r, t, slot):
        late, i, n_run, pair, na, nb, nc = run_of(r)
        n, tt = place(n_run, pair, t)
        in_a = tt < na
        in_c = tt >= na + nb
        in_b = jnp.logical_not(in_a) & jnp.logical_not(in_c)
        u = jnp.where(in_a, tt, jnp.where(in_c, tt - na - nb, tt - na))
        nk = jnp.where(in_a, na, jnp.where(in_c, nc, nb))
        full = (is_c & in_a) | (is_d & in_b) | (is_b & late & in_b)
        low = jnp.minimum(nk, 2)
        own = jnp.where(c == 0, low, nk - low)
        mine = (full & (u % 2 == 0)) | (jnp.logical_not(full) & (u < own))
        idx = jnp.where(full, u // 2, jnp.where(mine, u, u - own))
        kt = jnp.where(mine, 2 * c, 2 * (1 - c)) + idx
        k_strip = jnp.where(is_b & late, jnp.where(in_c, 6 + i, 4 + i), i)
        first = (n == 0) & jnp.logical_not(is_a & late)
        split = is_d & (i == 7)

        @pl.when(first & jnp.logical_not(in_a) & (u == 0))
        def _():
            with jax.named_scope('wait_rail'):
                arrive(k_strip, own)

        @pl.when(first & in_b & split & (u == 2))
        def _():
            with jax.named_scope('wait_rail_last'):
                send_l(l_ref, 7, 7, 8, across, KT, KT).wait_recv()
                lb_copy(7, KT, KT).start()

        @pl.when(first & jnp.logical_not(mine) & (idx == 0))
        def _():
            with jax.named_scope('wait_peer'):
                @pl.when(in_a)
                def _():
                    la_copy(i).wait_recv()

                @pl.when(jnp.logical_not(in_a))
                def _():
                    wait_peer(k_strip)

        @pl.when(first & in_b & split & (u == 3))
        def _():
            lb_copy(7, KT, KT).wait_recv()

        @pl.when(is_a & late & (i == 4) & (n == 0) & (u == 0))
        def _():
            with jax.named_scope('relay'):
                for j in range(2):
                    send_l(l_ref, j, j, j, along).wait_recv()
                    relay(j).start()

        @pl.when(((is_a & late & (i == 4)) | (is_c & in_a & (i == 0)) | (is_d & in_b & (i == 2))) & (u == 0))
        def _():
            with jax.named_scope('wait_b'):
                send_b(n, n, along).wait_recv()

        @pl.when(in_c & (i == 0) & (n == 0))
        def _():
            with jax.named_scope('wait_b'):
                send_b_top().wait_recv()

        use_rem = (is_a & late) | (is_c & in_a) | (is_d & in_b) | in_c
        rows = pl.ds(pl.multiple_of(k_strip * S, S), S)
        cols = pl.ds(pl.multiple_of((kt % 2) * KT, KT), KT)
        for take, ref in (
            (in_a & mine, l_ref),
            (in_a & jnp.logical_not(mine), lap),
            (jnp.logical_not(in_a) & mine, lbr),
            (jnp.logical_not(in_a) & jnp.logical_not(mine), lbp),
        ):
            @pl.when(take)
            def _():
                pltpu.make_async_copy(ref.at[rows, cols], lt.at[slot], lsem.at[slot]).start()
        depth = pl.ds(pl.multiple_of(kt * KT, KT), KT)
        ncols = pl.ds(pl.multiple_of(n * NT, NT), NT)
        for take, ref in ((use_rem, brem), (jnp.logical_not(use_rem), b_ref)):
            @pl.when(take)
            def _():
                pltpu.make_async_copy(ref.at[depth, ncols], bt.at[slot], bsem.at[slot]).start()

    def finish(r, n):
        late, i, _, _, _, _, _ = run_of(r)
        pltpu.make_async_copy(ot, x_ref.at[pl.ds(0, S), pl.ds(0, NT)], osem).wait()

        @pl.when(late)
        def _():
            send_x(i, n, jnp.where(is_a, r - 16, r - 8)).start()

    steps = pick(68, 32, 104, 84)
    fetch(jnp.int32(0), jnp.int32(0), 0)

    def step(s, state):
        r, t, waiting, r_old, n_old = state
        late, i, n_run, pair, na, nb, nc = run_of(r)
        n, tt = place(n_run, pair, t)
        total = na + nb + nc
        ends = t + 1 == jnp.where(pair, 2 * total, total)
        r_next = jnp.where(ends, r + 1, r)
        t_next = jnp.where(ends, 0, t + 1)
        slot = s % 2
        last = tt + 1 == total

        @pl.when(s + 1 < steps)
        def _():
            fetch(r_next, t_next, 1 - slot)

        @pl.when(tt == 0)
        def _():
            acc[n] = jnp.zeros_like(acc[n])

        pltpu.make_async_copy(l_ref.at[pl.ds(0, S), pl.ds(0, KT)], lt.at[slot], lsem.at[slot]).wait()
        pltpu.make_async_copy(b_ref.at[pl.ds(0, KT), pl.ds(0, NT)], bt.at[slot], bsem.at[slot]).wait()
        with jax.named_scope('dot'):
            acc[n] += jnp.dot(lt[slot], bt[slot], preferred_element_type=jnp.float32)

        @pl.when(waiting == 1)
        def _():
            finish(r_old, n_old)

        @pl.when(last)
        def _():
            ot[...] = acc[n].astype(ot.dtype)
            rows = pl.ds(pl.multiple_of(i * S, S), S)
            staged = pl.ds(pl.multiple_of(i % 4 * S, S), S)
            cols = pl.ds(pl.multiple_of(n * NT, NT), NT)

            @pl.when(late)
            def _():
                pltpu.make_async_copy(ot, xst.at[staged, cols], osem).start()

            @pl.when(jnp.logical_not(late))
            def _():
                pltpu.make_async_copy(ot, x_ref.at[rows, cols], osem).start()
        return r_next, t_next, jnp.where(last, 1, 0), r, n

    zero = jnp.int32(0)
    state = lax.fori_loop(0, steps, step, (zero, zero, zero, zero, zero))
    finish(state[3], state[4])

    @pl.when(is_a)
    def _():
        for j in range(2):
            relay(j).wait_send()
        for k in range(8):
            send_x(4 + k % 4, k // 4, k).wait_send()

    @pl.when(is_b)
    def _():
        with jax.named_scope('wait_x_sent'):
            for k in range(4):
                send_x(k % 2, k // 2, k).wait_send()
        with jax.named_scope('wait_x_in'):
            for k in range(8):
                send_x(4 + k % 4, k // 4, k).wait_recv()

    @pl.when(is_d)
    def _():
        with jax.named_scope('wait_x_in'):
            for k in range(4):
                send_x(k % 2, k // 2, k).wait_recv()

    with jax.named_scope('wait_own_sends'):
        own_sends(lambda copy: copy.wait_send())

    @pl.when(jnp.logical_not(is_a))
    def _():
        @pl.when(is_b)
        def _():
            for k in (4, 5):
                lb_copy(k).wait_send()

            @pl.when(c == 0)
            def _():
                for k in (0, 1, 2, 3, 6, 7):
                    lb_copy(k).wait_send()

        @pl.when(is_c)
        def _():
            @pl.when(c == 0)
            def _():
                for k in range(4):
                    lb_copy(k).wait_send()
            for k in range(4, 8):
                lb_copy(k).wait_send()

        @pl.when(is_d)
        def _():
            for k in range(2, 7):
                lb_copy(k).wait_send()
            lb_copy(7, 0, KT).wait_send()
            lb_copy(7, KT, KT).wait_send()


def solution(mesh):
    block_spec = P(('batch', 'row'), 'col')

    def local_product(l_block, b_block):
        rows, half = l_block.shape
        columns = b_block.shape[1]
        l_like = jax.ShapeDtypeStruct((rows, half), l_block.dtype)
        b_like = jax.ShapeDtypeStruct((rows, columns), b_block.dtype)
        x_like = jax.ShapeDtypeStruct((rows // 2, columns), b_block.dtype)
        dma = pltpu.SemaphoreType.DMA
        out = pl.pallas_call(
            kernel,
            out_shape=[b_like, l_like, l_like, l_like, b_like, x_like],
            in_specs=[pl.BlockSpec(memory_space=pl.ANY)] * 2,
            out_specs=[pl.BlockSpec(memory_space=pl.ANY)] * 6,
            scratch_shapes=[
                pltpu.VMEM((2, S, KT), l_block.dtype),
                pltpu.VMEM((2, KT, NT), b_block.dtype),
                pltpu.VMEM((2, S, NT), jnp.float32),
                pltpu.VMEM((S, NT), b_block.dtype),
                dma((2,)), dma((2,)), dma, dma,
                dma((4,)), dma((2,)), dma((10,)), dma((9,)),
                dma((8,)), dma((8,)), dma((9,)), dma((9,)), dma((8,)), dma((8,)),
            ],
            compiler_params=pltpu.CompilerParams(
                collective_id=0, has_side_effects=True, vmem_limit_bytes=48 * 2**20),
            name='triangular_product',
        )(l_block, b_block)
        return out[0]

    return jax.shard_map(local_product, mesh=mesh, in_specs=(block_spec, block_spec),
                         out_specs=block_spec, check_vma=False)
```

```python
import jax
import jax.numpy as jnp
from jax import lax
from jax.experimental import pallas as pl
from jax.experimental.pallas import tpu as pltpu
from jax.sharding import PartitionSpec as P

MESH = pl.DeviceIdType.MESH
S = 896
KT = 1792
NT = 1024
Q = 224


def kernel(l_ref, b_ref, x_ref, lap, lbr, lbp, brem, xst, pst, lt, bt, acc, ot,
           lsem, bsem, osem, psem, zsem, bs, br, ls, lr, ps, pr, qs, qr, xs, xr):
    batch, row, col = lax.axis_index('batch'), lax.axis_index('row'), lax.axis_index('col')
    x, c = col // 2, col % 2
    is_a = (row == 0) & (x == 0)
    is_b = (row == 0) & (x == 1)
    is_c = (row == 1) & (x == 0)
    is_d = (row == 1) & (x == 1)
    half = l_ref.shape[1]
    peer = (batch, row, 2 * x + 1 - c)
    across = (batch, row, 2 * (1 - x) + c)
    along = (batch, 1 - row, col)

    barrier = pltpu.get_barrier_semaphore()
    for device in (peer, across, along):
        pl.semaphore_signal(barrier, inc=1, device_id=device, device_id_type=MESH)
    pl.semaphore_wait(barrier, 3)

    def remote(src, dst, send, recv, device):
        return pltpu.make_async_remote_copy(
            src_ref=src, dst_ref=dst, send_sem=send, recv_sem=recv,
            device_id=device, device_id_type=MESH)

    def strip(i, lo=0, width=None):
        return pl.ds(i * S, S), pl.ds(lo, half if width is None else width)

    def send_l(src, i, k, out, device, lo=0, width=None):
        return remote(src.at[strip(i, lo, width)], lbr.at[strip(k, lo, width)],
                      ls.at[out], lr.at[k if lo == 0 else 8], device)

    def tri_width(i, h):
        return min((i + 1) * S - h * half, half)

    def send_tri(i, h):
        return send_l(l_ref, i, i, i, across, 0, tri_width(i, h))

    def send_b(n, out, device):
        cols = pl.ds(n * NT, NT)
        return remote(b_ref.at[:, cols], brem.at[:, cols], bs.at[out], br.at[n], device)

    def send_b_top(j):
        rows = pl.ds(j * KT, KT)
        return remote(b_ref.at[rows], brem.at[rows], bs.at[j], br.at[j], along)

    def send_rows(src, at, to, rows, k, out, device):
        return remote(src.at[pl.ds(at, rows)], lbr.at[pl.ds(to, rows)], ls.at[out], lr.at[k], device)

    def send_rest():
        return send_rows(l_ref, 2 * S + Q, 2 * S + Q, S - Q, 2, 9, across)

    def send_c(i):
        if i < 2:
            return [send_l(l_ref, i, i, i, along)]
        if i == 2:
            return [send_rows(l_ref, 2 * S, 2 * S, Q, 2, 2, along), send_rest()]
        if i < 7:
            return [send_l(l_ref, i, i, i, across)]
        return [send_l(l_ref, i, i, 7, across, 0, KT), send_l(l_ref, i, i, 8, across, KT, KT)]

    def relay(j):
        if j == 2:
            return send_rows(lbr, 2 * S, 8 * S, Q, 8, 10, across)
        return send_l(lbr, j, 4 + j, 8 + j, across)

    def send_l11_top(j):
        if j == 2:
            return send_rows(l_ref, 2 * S, 9 * S, Q, 9, 10, along)
        return send_l(l_ref, j, 6 + j, 8 + j, along, 0, tri_width(j, 0))

    def la_copy(i):
        rows = pl.ds(i * S, S)
        return remote(l_ref.at[rows], lap.at[rows], ps.at[i], pr.at[i], peer)

    def lb_copy(i, lo=0, width=None):
        at = strip(i, lo, width)
        k = i if lo == 0 else 8
        return remote(lbr.at[at], lbp.at[at], qs.at[k], qr.at[k], peer)

    def send_x(i, n, k):
        cols = pl.ds(pl.multiple_of(n * NT, NT), NT)
        src = pl.ds(pl.multiple_of(i % 4 * S, S), S)
        dst = pl.ds(pl.multiple_of(i * S, S), S)
        target = (batch, jnp.where(is_a, row, 1 - row), jnp.where(is_a, 2 * (1 - x) + c, col))
        return remote(xst.at[src, cols], x_ref.at[dst, cols], xs.at[k], xr.at[k], target)

    def send_x_head(n, k):
        cols = pl.ds(pl.multiple_of(n * NT, NT), NT)
        at = (pl.ds(2 * S, Q), cols)
        return remote(xst.at[at], x_ref.at[at], xs.at[k], xr.at[k], along)

    def send_tile_b(k):
        j, n = k % 3, k // 3
        return send_x_head(n, k) if j == 2 else send_x(j, n, k)

    def each_tri(do):
        for h in (0, 1):
            @pl.when(c == h)
            def _():
                for i in range(4 * h, 8):
                    do(i, h)

    def each_la(do):
        @pl.when(is_c | (is_a & (c == 0)))
        def _():
            for i in range(2):
                do(i)

        @pl.when(is_c | (c == 0))
        def _():
            for i in range(2, 4):
                do(i)
        for i in range(4, 8):
            do(i)

    def own_sends(do):
        @pl.when(is_a)
        def _():
            for n in range(2):
                do(send_b(n, n, along))

            @pl.when(c == 0)
            def _():
                for i in range(4):
                    do(send_tri(i, 0))

        @pl.when(is_b)
        def _():
            for n in range(2):
                do(send_b(n, n, along))
                do(send_b(n, 2 + n, across))

        @pl.when(is_c)
        def _():
            for i in range(8):
                for copy in send_c(i):
                    do(copy)

        @pl.when(is_d)
        def _():
            @pl.when(c == 0)
            def _():
                for j in range(3):
                    do(send_l11_top(j))
            for j in range(2):
                do(send_b_top(j))
            each_tri(lambda i, h: do(send_tri(i, h)))

        @pl.when(jnp.logical_not(is_b))
        def _():
            each_la(lambda i: do(la_copy(i)))

    own_sends(lambda copy: copy.start())

    def zero_corner(k, j):
        @pl.when((is_c & (c == k // 4)) | (is_b & (c == 0) & (k != 4)))
        def _():
            cols = pl.ds((1 if k in (0, 4) or j == 6 else 3) * S, S)
            copy = pltpu.make_async_copy(ot.at[:, pl.ds(0, S)], lbr.at[pl.ds(k * S, S), cols], zsem)
            copy.start()
            copy.wait()

    @pl.when(is_b | is_c)
    def _():
        ot[...] = jnp.zeros_like(ot)
        for k in (0, 2, 4):
            zero_corner(k, k)

        @pl.when(is_c & (c == 1))
        def _():
            copy = pltpu.make_async_copy(
                ot.at[:, pl.ds(0, S)], lbr.at[pl.ds(6 * S, S), pl.ds(3 * S, S)], zsem)
            copy.start()
            copy.wait()

        @pl.when(is_b & (c == 0))
        def _():
            copy = pltpu.make_async_copy(
                ot.at[:, pl.ds(0, S)], lbr.at[pl.ds(6 * S, S), pl.ds(S, S)], zsem)
            copy.start()
            copy.wait()

    def pick(a, b, c_, d):
        return jnp.where(is_a, a, jnp.where(is_b, b, jnp.where(is_c, c_, d)))

    def run_of(r):
        late = pick(r >= 16, r >= 8, False, False)
        part = pick(False, False, (r < 3) | ((r >= 6) & (r < 14) & (r % 2 == 1)), r < 8)
        rest = pick(False, False, (r >= 15) & (r < 22), r >= 12)
        pair = is_d & (r >= 16)
        i_c = jnp.where(r < 3, r, jnp.where(r < 6, r - 3, jnp.where(
            r < 15, r // 2, jnp.where(r < 22, r - 15, 7))))
        n_c = jnp.where(r < 3, 1, jnp.where(r < 6, 0, jnp.where(r < 15, r % 2, 1)))
        i_d = jnp.where(r < 4, 2 + r, jnp.where(r < 8, 4 + r // 2, jnp.where(r < 16, 2 + r % 4, r - 10)))
        n_d = jnp.where(r < 4, 1, jnp.where(r < 8, r % 2, jnp.where(r < 12, 0, jnp.where(r < 16, 1, 0))))
        i = pick(jnp.where(late, 4 + r % 4, r % 8), jnp.where(late, (r - 8) % 3, r % 4), i_c, i_d)
        n = pick(jnp.where(late, (r - 16) // 4, r // 8), jnp.where(late, (r - 8) // 3, r // 4), n_c, n_d)
        tri = i // 2 + 1
        na = pick(tri, 0, jnp.where(part, 0, 4), jnp.where(rest, 0, tri))
        nb = pick(0, jnp.where(late, 4, tri), jnp.where(rest, 0, tri), jnp.where(part, 0, 4))
        nc = jnp.where(is_b & late, 1 + i // 2, 0)
        return late, part, rest, i, n, pair, na, nb, nc

    def kept(r, i, n):
        k = jnp.where(is_c, i, jnp.where(r < 8, r, jnp.where(r < 16, r - 12, 2 * i - 8 + n)))
        return pst.at[pl.ds(pl.multiple_of(k * S, S), S)]

    def acc_of(r, pair, n):
        return jnp.where(pair, n, r % 2)

    def place(n, pair, t):
        return jnp.where(pair, t % 2, n), jnp.where(pair, t // 2, t)

    def arrive(k_dyn, own):
        for k in range(8):
            @pl.when(k_dyn == k)
            def _():
                @pl.when(is_d)
                def _():
                    if k == 2:
                        send_rest().wait_recv()
                    elif k < 7:
                        send_l(l_ref, k, k, k, across).wait_recv()
                    else:
                        send_l(l_ref, k, k, k, across, 0, KT).wait_recv()

                @pl.when(is_c)
                def _():
                    for h in (0, 1):
                        if k >= 4 * h:
                            @pl.when(c == h)
                            def _():
                                send_tri(k, h).wait_recv()

                @pl.when(is_b)
                def _():
                    if k in (4, 5):
                        send_l(l_ref, k, k, k, across).wait_recv()
                    else:
                        @pl.when(c == 0)
                        def _():
                            send_l(l_ref, k, k, k, across, 0, tri_width(k % 6, 0)).wait_recv()

                pass_on(k, own)

        @pl.when(is_b)
        def _():
            for k in (8, 9):
                @pl.when((k_dyn == k) & (own > 0))
                def _():
                    send_rows(l_ref, 0, k * S, Q, k, 0, across).wait_recv()
                    lb_copy(k).start()

    def pass_on(k, own):
                @pl.when(own > 0)
                def _():
                    if k < 7:
                        lb_copy(k).start()
                    else:
                        @pl.when(is_d)
                        def _():
                            lb_copy(k, 0, KT).start()

                        @pl.when(jnp.logical_not(is_d))
                        def _():
                            lb_copy(k).start()

    def wait_peer(k_dyn):
        @pl.when(is_b)
        def _():
            for k in (8, 9):
                @pl.when(k_dyn == k)
                def _():
                    lb_copy(k).wait_recv()

        for k in range(8):
            @pl.when(k_dyn == k)
            def _():
                if k < 7:
                    lb_copy(k).wait_recv()
                else:
                    @pl.when(is_d)
                    def _():
                        lb_copy(k, 0, KT).wait_recv()

                    @pl.when(jnp.logical_not(is_d))
                    def _():
                        lb_copy(k).wait_recv()

    def fetch(r, t, slot):
        late, _, rest, i, n_run, pair, na, nb, nc = run_of(r)
        n, tt = place(n_run, pair, t)
        in_a = tt < na
        in_c = tt >= na + nb
        in_b = jnp.logical_not(in_a) & jnp.logical_not(in_c)
        u = jnp.where(in_a, tt, jnp.where(in_c, tt - na - nb, tt - na))
        nk = jnp.where(in_a, na, jnp.where(in_c, nc, nb))
        full = (is_c & in_a) | (is_d & in_b) | (is_b & late & in_b)
        low = jnp.minimum(nk, 2)
        own = jnp.where(c == 0, low, nk - low)
        mine = (full & (u % 2 == 0)) | (jnp.logical_not(full) & (u < own))
        idx = jnp.where(full, u // 2, jnp.where(mine, u, u - own))
        kt = jnp.where(mine, 2 * c, 2 * (1 - c)) + idx
        k_strip = jnp.where(is_b & late, jnp.where(
            i == 2, jnp.where(in_c, 9, 8), jnp.where(in_c, 6 + i, 4 + i)), i)
        first = pick((n == 0) & jnp.logical_not(late), n == 0,
                     (in_a & (n == 0)) | (jnp.logical_not(in_a) & ((r < 3) | ((r >= 6) & (r < 15) & (r % 2 == 0)))),
                     jnp.where(in_a, (r < 5) | (r == 6), n == 0))
        split = is_d & (i == 7)

        @pl.when(first & jnp.logical_not(in_a) & (u == 0))
        def _():
            with jax.named_scope('wait_rail'):
                arrive(k_strip, own)

        @pl.when(first & in_b & split & (u == 2))
        def _():
            with jax.named_scope('wait_rail_last'):
                send_l(l_ref, 7, 7, 8, across, KT, KT).wait_recv()
                lb_copy(7, KT, KT).start()

        @pl.when(first & jnp.logical_not(mine) & (idx == 0))
        def _():
            with jax.named_scope('wait_peer'):
                @pl.when(in_a)
                def _():
                    la_copy(i).wait_recv()

                @pl.when(jnp.logical_not(in_a))
                def _():
                    wait_peer(k_strip)

        @pl.when(first & in_b & split & (u == 3))
        def _():
            lb_copy(7, KT, KT).wait_recv()

        @pl.when(is_a & late & (i == 4) & (n == 0) & (u == 0))
        def _():
            with jax.named_scope('relay'):
                for j in range(3):
                    send_c(j)[0].wait_recv()
                    relay(j).start()

        @pl.when(((is_a & late & (i == 4)) | (is_c & in_a & (i == 0)) | (is_d & in_b & (i == 2))) & (u == 0))
        def _():
            with jax.named_scope('wait_b'):
                send_b(n, n, along).wait_recv()

        for j in range(2):
            @pl.when(in_c & (i == 2 * j) & (n == 0) & (u == 0))
            def _():
                with jax.named_scope('wait_b'):
                    send_b_top(j).wait_recv()

        @pl.when(rest & (tt == 0))
        def _():
            k = acc_of(r, pair, n)
            pltpu.make_async_copy(kept(r, i, n), acc.at[k], psem.at[k]).start()

        use_rem = (is_a & late) | (is_c & in_a) | (is_d & in_b) | in_c
        rows = pl.ds(pl.multiple_of(k_strip * S, S), S)
        cols = pl.ds(pl.multiple_of((kt % 2) * KT, KT), KT)
        for take, ref in (
            (in_a & mine, l_ref),
            (in_a & jnp.logical_not(mine), lap),
            (jnp.logical_not(in_a) & mine, lbr),
            (jnp.logical_not(in_a) & jnp.logical_not(mine), lbp),
        ):
            @pl.when(take)
            def _():
                pltpu.make_async_copy(ref.at[rows, cols], lt.at[slot], lsem.at[slot]).start()
        depth = pl.ds(pl.multiple_of(kt * KT, KT), KT)
        ncols = pl.ds(pl.multiple_of(n * NT, NT), NT)
        for take, ref in ((use_rem, brem), (jnp.logical_not(use_rem), b_ref)):
            @pl.when(take)
            def _():
                pltpu.make_async_copy(ref.at[depth, ncols], bt.at[slot], bsem.at[slot]).start()

    def finish(r, n):
        late, part, _, i, _, _, _, _, _ = run_of(r)
        head = is_d & (i == 2) & jnp.logical_not(part)

        @pl.when(part)
        def _():
            pltpu.make_async_copy(acc.at[0], pst.at[pl.ds(0, S)], osem).wait()

        @pl.when(head)
        def _():
            pltpu.make_async_copy(ot.at[pl.ds(Q, S - Q)], x_ref.at[pl.ds(0, S - Q), pl.ds(0, NT)], osem).wait()

        @pl.when(jnp.logical_not(part | head))
        def _():
            pltpu.make_async_copy(ot, x_ref.at[pl.ds(0, S), pl.ds(0, NT)], osem).wait()

        @pl.when(late & is_b & (i == 2))
        def _():
            send_x_head(n, r - 8).start()

        @pl.when(late & jnp.logical_not(is_b & (i == 2)))
        def _():
            send_x(i, n, jnp.where(is_a, r - 16, r - 8)).start()

    steps = pick(68, 44, 104, 84)
    fetch(jnp.int32(0), jnp.int32(0), 0)

    def step(s, state):
        r, t, waiting, r_old, n_old = state
        late, part, rest, i, n_run, pair, na, nb, nc = run_of(r)
        n, tt = place(n_run, pair, t)
        total = na + nb + nc
        ends = t + 1 == jnp.where(pair, 2 * total, total)
        r_next = jnp.where(ends, r + 1, r)
        t_next = jnp.where(ends, 0, t + 1)
        slot = s % 2
        last = tt + 1 == total
        k = acc_of(r, pair, n)
        late_old = pick(r_old >= 16, r_old >= 8, False, False)

        @pl.when((waiting == 1) & late_old)
        def _():
            finish(r_old, n_old)

        stalls = (is_a & (r_next == 20) & (t_next == 0)) | (is_d & (r_next == 17) & (t_next == 4))

        @pl.when((s + 1 < steps) & jnp.logical_not(stalls))
        def _():
            fetch(r_next, t_next, 1 - slot)

        @pl.when((tt == 0) & rest)
        def _():
            pltpu.make_async_copy(pst.at[pl.ds(0, S)], acc.at[k], psem.at[k]).wait()

        @pl.when((tt == 0) & jnp.logical_not(rest))
        def _():
            acc[k] = jnp.zeros_like(acc[k])

        pltpu.make_async_copy(l_ref.at[pl.ds(0, S), pl.ds(0, KT)], lt.at[slot], lsem.at[slot]).wait()
        pltpu.make_async_copy(b_ref.at[pl.ds(0, KT), pl.ds(0, NT)], bt.at[slot], bsem.at[slot]).wait()
        with jax.named_scope('dot'):
            acc[k] += jnp.dot(lt[slot], bt[slot], preferred_element_type=jnp.float32)

        @pl.when((waiting == 1) & jnp.logical_not(late_old))
        def _():
            finish(r_old, n_old)

        @pl.when(last & part)
        def _():
            pltpu.make_async_copy(acc.at[k], kept(r, i, n), osem).start()

        @pl.when(last & jnp.logical_not(part))
        def _():
            ot[...] = acc[k].astype(ot.dtype)
            rows = pl.ds(pl.multiple_of(i * S, S), S)
            staged = pl.ds(pl.multiple_of(i % 4 * S, S), S)
            cols = pl.ds(pl.multiple_of(n * NT, NT), NT)
            head = is_d & (i == 2)

            @pl.when(late)
            def _():
                pltpu.make_async_copy(ot, xst.at[staged, cols], osem).start()

            @pl.when(head)
            def _():
                pltpu.make_async_copy(
                    ot.at[pl.ds(Q, S - Q)], x_ref.at[pl.ds(2 * S + Q, S - Q), cols], osem).start()

            @pl.when(jnp.logical_not(late | head))
            def _():
                pltpu.make_async_copy(ot, x_ref.at[rows, cols], osem).start()
        @pl.when(stalls)
        def _():
            @pl.when(last)
            def _():
                finish(r, n)
            fetch(r_next, t_next, 1 - slot)
        return r_next, t_next, jnp.where(last & jnp.logical_not(stalls), 1, 0), r, n

    zero = jnp.int32(0)
    state = lax.fori_loop(0, steps, step, (zero, zero, zero, zero, zero))
    finish(state[3], state[4])

    @pl.when(is_a)
    def _():
        for j in range(3):
            relay(j).wait_send()
        for k in range(8):
            send_x(4 + k % 4, k // 4, k).wait_send()

    @pl.when(is_b)
    def _():
        for k in range(8):
            with jax.named_scope('wait_x_in'):
                send_x(4 + k % 4, k // 4, k).wait_recv()
        with jax.named_scope('wait_x_sent'):
            for k in range(6):
                send_tile_b(k).wait_send()

    @pl.when(is_d)
    def _():
        with jax.named_scope('wait_x_in'):
            for k in range(6):
                send_tile_b(k).wait_recv()

    with jax.named_scope('wait_own_sends'):
        own_sends(lambda copy: copy.wait_send())

    @pl.when(jnp.logical_not(is_a))
    def _():
        @pl.when(is_b)
        def _():
            for k in (4, 5, 8):
                lb_copy(k).wait_send()

            @pl.when(c == 0)
            def _():
                for k in (0, 1, 2, 3, 6, 7, 9):
                    lb_copy(k).wait_send()

        @pl.when(is_c)
        def _():
            @pl.when(c == 0)
            def _():
                for k in range(4):
                    lb_copy(k).wait_send()
            for k in range(4, 8):
                lb_copy(k).wait_send()

        @pl.when(is_d)
        def _():
            for k in range(2, 7):
                lb_copy(k).wait_send()
            lb_copy(7, 0, KT).wait_send()
            lb_copy(7, KT, KT).wait_send()


def solution(mesh):
    block_spec = P(('batch', 'row'), 'col')

    def local_product(l_block, b_block):
        rows, half = l_block.shape
        columns = b_block.shape[1]
        l_like = jax.ShapeDtypeStruct((rows, half), l_block.dtype)
        l_more = jax.ShapeDtypeStruct((rows + 2 * S, half), l_block.dtype)
        b_like = jax.ShapeDtypeStruct((rows, columns), b_block.dtype)
        x_like = jax.ShapeDtypeStruct((rows // 2, columns), b_block.dtype)
        part_like = jax.ShapeDtypeStruct((8 * S, NT), jnp.float32)
        dma = pltpu.SemaphoreType.DMA
        out = pl.pallas_call(
            kernel,
            out_shape=[b_like, l_like, l_more, l_more, b_like, x_like, part_like],
            in_specs=[pl.BlockSpec(memory_space=pl.ANY)] * 2,
            out_specs=[pl.BlockSpec(memory_space=pl.ANY)] * 7,
            scratch_shapes=[
                pltpu.VMEM((2, S, KT), l_block.dtype),
                pltpu.VMEM((2, KT, NT), b_block.dtype),
                pltpu.VMEM((2, S, NT), jnp.float32),
                pltpu.VMEM((S, NT), b_block.dtype),
                dma((2,)), dma((2,)), dma, dma((2,)), dma,
                dma((4,)), dma((2,)), dma((11,)), dma((10,)),
                dma((8,)), dma((8,)), dma((10,)), dma((10,)), dma((8,)), dma((8,)),
            ],
            compiler_params=pltpu.CompilerParams(
                collective_id=0, has_side_effects=True, vmem_limit_bytes=48 * 2**20),
            name='triangular_product',
        )(l_block, b_block)
        return out[0]

    return jax.shard_map(local_product, mesh=mesh, in_specs=(block_spec, block_spec),
                         out_specs=block_spec, check_vma=False)
```

```python
import jax
import jax.numpy as jnp
from jax import lax
from jax.experimental import pallas as pl
from jax.experimental.pallas import tpu as pltpu
from jax.sharding import PartitionSpec as P

MESH = pl.DeviceIdType.MESH
S = 896
KT = 1792
NT = 1024
Q = 240


def kernel(l_ref, b_ref, x_ref, lap, lbr, lbp, brem, xst, pst, lt, bt, acc, ot,
           lsem, bsem, osem, psem, zsem, bs, br, ls, lr, ps, pr, qs, qr, xs, xr):
    batch, row, col = lax.axis_index('batch'), lax.axis_index('row'), lax.axis_index('col')
    x, c = col // 2, col % 2
    is_a = (row == 0) & (x == 0)
    is_b = (row == 0) & (x == 1)
    is_c = (row == 1) & (x == 0)
    is_d = (row == 1) & (x == 1)
    half = l_ref.shape[1]
    peer = (batch, row, 2 * x + 1 - c)
    across = (batch, row, 2 * (1 - x) + c)
    along = (batch, 1 - row, col)

    barrier = pltpu.get_barrier_semaphore()
    for device in (peer, across, along):
        pl.semaphore_signal(barrier, inc=1, device_id=device, device_id_type=MESH)
    pl.semaphore_wait(barrier, 3)

    def remote(src, dst, send, recv, device):
        return pltpu.make_async_remote_copy(
            src_ref=src, dst_ref=dst, send_sem=send, recv_sem=recv,
            device_id=device, device_id_type=MESH)

    def strip(i, lo=0, width=None):
        return pl.ds(i * S, S), pl.ds(lo, half if width is None else width)

    def send_l(src, i, k, out, device, lo=0, width=None):
        return remote(src.at[strip(i, lo, width)], lbr.at[strip(k, lo, width)],
                      ls.at[out], lr.at[k if lo == 0 else 8], device)

    def tri_width(i, h):
        return min((i + 1) * S - h * half, half)

    def send_tri(i, h):
        return send_l(l_ref, i, i, i, across, 0, tri_width(i, h))

    def send_b(n, out, device):
        cols = pl.ds(n * NT, NT)
        return remote(b_ref.at[:, cols], brem.at[:, cols], bs.at[out], br.at[n], device)

    def send_b_top(j):
        rows = pl.ds(j * KT, KT)
        return remote(b_ref.at[rows], brem.at[rows], bs.at[j], br.at[j], along)

    def send_rows(src, at, to, rows, k, out, device):
        return remote(src.at[pl.ds(at, rows)], lbr.at[pl.ds(to, rows)], ls.at[out], lr.at[k], device)

    def send_rest():
        return send_rows(l_ref, 2 * S + Q, 2 * S + Q, S - Q, 2, 9, across)

    def send_c(i):
        if i < 2:
            return [send_l(l_ref, i, i, i, along)]
        if i == 2:
            return [send_rows(l_ref, 2 * S, 2 * S, Q, 2, 2, along), send_rest()]
        if i < 7:
            return [send_l(l_ref, i, i, i, across)]
        return [send_l(l_ref, i, i, 7, across, 0, KT), send_l(l_ref, i, i, 8, across, KT, KT)]

    def relay(j):
        if j == 2:
            return send_rows(lbr, 2 * S, 8 * S, Q, 8, 10, across)
        return send_l(lbr, j, 4 + j, 8 + j, across)

    def send_l11_top(j):
        if j == 2:
            return send_rows(l_ref, 2 * S, 9 * S, Q, 9, 10, along)
        return send_l(l_ref, j, 6 + j, 8 + j, along, 0, tri_width(j, 0))

    def la_copy(i):
        rows = pl.ds(i * S, S)
        return remote(l_ref.at[rows], lap.at[rows], ps.at[i], pr.at[i], peer)

    def lb_copy(i, lo=0, width=None):
        at = strip(i, lo, width)
        k = i if lo == 0 else 8
        return remote(lbr.at[at], lbp.at[at], qs.at[k], qr.at[k], peer)

    def send_x(i, n, k):
        cols = pl.ds(pl.multiple_of(n * NT, NT), NT)
        src = pl.ds(pl.multiple_of(i % 4 * S, S), S)
        dst = pl.ds(pl.multiple_of(i * S, S), S)
        target = (batch, jnp.where(is_a, row, 1 - row), jnp.where(is_a, 2 * (1 - x) + c, col))
        return remote(xst.at[src, cols], x_ref.at[dst, cols], xs.at[k], xr.at[k], target)

    def send_x_head(n, k):
        cols = pl.ds(pl.multiple_of(n * NT, NT), NT)
        at = (pl.ds(2 * S, Q), cols)
        return remote(xst.at[at], x_ref.at[at], xs.at[k], xr.at[k], along)

    def send_tile_b(k):
        j, n = k % 3, k // 3
        return send_x_head(n, k) if j == 2 else send_x(j, n, k)

    def each_tri(do):
        for h in (0, 1):
            @pl.when(c == h)
            def _():
                for i in range(4 * h, 8):
                    do(i, h)

    def each_la(do):
        @pl.when(is_c | (is_a & (c == 0)))
        def _():
            for i in range(2):
                do(i)

        @pl.when(is_c | (c == 0))
        def _():
            for i in range(2, 4):
                do(i)
        for i in range(4, 8):
            do(i)

    def own_sends(do):
        @pl.when(is_a)
        def _():
            for n in range(2):
                do(send_b(n, n, along))

            @pl.when(c == 0)
            def _():
                for i in range(4):
                    do(send_tri(i, 0))

        @pl.when(is_b)
        def _():
            for n in range(2):
                do(send_b(n, n, along))
                do(send_b(n, 2 + n, across))

        @pl.when(is_c)
        def _():
            for i in range(8):
                for copy in send_c(i):
                    do(copy)

        @pl.when(is_d)
        def _():
            @pl.when(c == 0)
            def _():
                for j in range(3):
                    do(send_l11_top(j))
            for j in range(2):
                do(send_b_top(j))
            each_tri(lambda i, h: do(send_tri(i, h)))

        @pl.when(jnp.logical_not(is_b))
        def _():
            each_la(lambda i: do(la_copy(i)))

    own_sends(lambda copy: copy.start())

    def zero_corner(k, j):
        @pl.when((is_c & (c == k // 4)) | (is_b & (c == 0) & (k != 4)))
        def _():
            cols = pl.ds((1 if k in (0, 4) or j == 6 else 3) * S, S)
            copy = pltpu.make_async_copy(ot.at[:, pl.ds(0, S)], lbr.at[pl.ds(k * S, S), cols], zsem)
            copy.start()
            copy.wait()

    @pl.when(is_b | is_c)
    def _():
        ot[...] = jnp.zeros_like(ot)
        for k in (0, 2, 4):
            zero_corner(k, k)

        @pl.when(is_c & (c == 1))
        def _():
            copy = pltpu.make_async_copy(
                ot.at[:, pl.ds(0, S)], lbr.at[pl.ds(6 * S, S), pl.ds(3 * S, S)], zsem)
            copy.start()
            copy.wait()

        @pl.when(is_b & (c == 0))
        def _():
            copy = pltpu.make_async_copy(
                ot.at[:, pl.ds(0, S)], lbr.at[pl.ds(6 * S, S), pl.ds(S, S)], zsem)
            copy.start()
            copy.wait()

    def pick(a, b, c_, d):
        return jnp.where(is_a, a, jnp.where(is_b, b, jnp.where(is_c, c_, d)))

    def run_of(r):
        late = pick(r >= 16, r >= 8, False, False)
        part = pick(False, False, (r < 3) | ((r >= 6) & (r < 14) & (r % 2 == 1)), r < 8)
        rest = pick(False, False, (r >= 15) & (r < 22), r >= 12)
        pair = is_d & (r >= 16)
        i_c = jnp.where(r < 3, r, jnp.where(r < 6, r - 3, jnp.where(
            r < 15, r // 2, jnp.where(r < 22, r - 15, 7))))
        n_c = jnp.where(r < 3, 1, jnp.where(r < 6, 0, jnp.where(r < 15, r % 2, 1)))
        i_d = jnp.where(r < 4, 2 + r, jnp.where(r < 8, 4 + r // 2, jnp.where(r < 16, 2 + r % 4, r - 10)))
        n_d = jnp.where(r < 4, 1, jnp.where(r < 8, r % 2, jnp.where(r < 12, 0, jnp.where(r < 16, 1, 0))))
        i = pick(jnp.where(late, 4 + r % 4, r % 8), jnp.where(late, (r - 8) % 3, r % 4), i_c, i_d)
        n = pick(jnp.where(late, (r - 16) // 4, r // 8), jnp.where(late, (r - 8) // 3, r // 4), n_c, n_d)
        tri = i // 2 + 1
        na = pick(tri, 0, jnp.where(part, 0, 4), jnp.where(rest, 0, tri))
        nb = pick(0, jnp.where(late, 4, tri), jnp.where(rest, 0, tri), jnp.where(part, 0, 4))
        nc = jnp.where(is_b & late, 1 + i // 2, 0)
        return late, part, rest, i, n, pair, na, nb, nc

    def kept(r, i, n):
        k = jnp.where(is_c, i, jnp.where(r < 8, r, jnp.where(r < 16, r - 12, 2 * i - 8 + n)))
        return pst.at[pl.ds(pl.multiple_of(k * S, S), S)]

    def acc_of(r, pair, n):
        return jnp.where(pair, n, r % 2)

    def place(n, pair, t):
        return jnp.where(pair, t % 2, n), jnp.where(pair, t // 2, t)

    def arrive(k_dyn, own):
        for k in range(8):
            @pl.when(k_dyn == k)
            def _():
                @pl.when(is_d)
                def _():
                    if k == 2:
                        send_rest().wait_recv()
                    elif k < 7:
                        send_l(l_ref, k, k, k, across).wait_recv()
                    else:
                        send_l(l_ref, k, k, k, across, 0, KT).wait_recv()

                @pl.when(is_c)
                def _():
                    for h in (0, 1):
                        if k >= 4 * h:
                            @pl.when(c == h)
                            def _():
                                send_tri(k, h).wait_recv()

                @pl.when(is_b)
                def _():
                    if k in (4, 5):
                        send_l(l_ref, k, k, k, across).wait_recv()
                    else:
                        @pl.when(c == 0)
                        def _():
                            send_l(l_ref, k, k, k, across, 0, tri_width(k % 6, 0)).wait_recv()

                pass_on(k, own)

        @pl.when(is_b)
        def _():
            for k in (8, 9):
                @pl.when((k_dyn == k) & (own > 0))
                def _():
                    send_rows(l_ref, 0, k * S, Q, k, 0, across).wait_recv()
                    lb_copy(k).start()

    def pass_on(k, own):
                @pl.when(own > 0)
                def _():
                    if k < 7:
                        lb_copy(k).start()
                    else:
                        @pl.when(is_d)
                        def _():
                            lb_copy(k, 0, KT).start()

                        @pl.when(jnp.logical_not(is_d))
                        def _():
                            lb_copy(k).start()

    def wait_peer(k_dyn):
        @pl.when(is_b)
        def _():
            for k in (8, 9):
                @pl.when(k_dyn == k)
                def _():
                    lb_copy(k).wait_recv()

        for k in range(8):
            @pl.when(k_dyn == k)
            def _():
                if k < 7:
                    lb_copy(k).wait_recv()
                else:
                    @pl.when(is_d)
                    def _():
                        lb_copy(k, 0, KT).wait_recv()

                    @pl.when(jnp.logical_not(is_d))
                    def _():
                        lb_copy(k).wait_recv()

    def fetch(r, t, slot):
        late, _, rest, i, n_run, pair, na, nb, nc = run_of(r)
        n, tt = place(n_run, pair, t)
        in_a = tt < na
        in_c = tt >= na + nb
        in_b = jnp.logical_not(in_a) & jnp.logical_not(in_c)
        u = jnp.where(in_a, tt, jnp.where(in_c, tt - na - nb, tt - na))
        nk = jnp.where(in_a, na, jnp.where(in_c, nc, nb))
        full = (is_c & in_a) | (is_d & in_b) | (is_b & late & in_b)
        low = jnp.minimum(nk, 2)
        own = jnp.where(c == 0, low, nk - low)
        mine = (full & (u % 2 == 0)) | (jnp.logical_not(full) & (u < own))
        idx = jnp.where(full, u // 2, jnp.where(mine, u, u - own))
        kt = jnp.where(mine, 2 * c, 2 * (1 - c)) + idx
        k_strip = jnp.where(is_b & late, jnp.where(
            i == 2, jnp.where(in_c, 9, 8), jnp.where(in_c, 6 + i, 4 + i)), i)
        first = pick((n == 0) & jnp.logical_not(late), n == 0,
                     (in_a & (n == 0)) | (jnp.logical_not(in_a) & ((r < 3) | ((r >= 6) & (r < 15) & (r % 2 == 0)))),
                     jnp.where(in_a, (r < 5) | (r == 6), n == 0))
        split = is_d & (i == 7)

        @pl.when(first & jnp.logical_not(in_a) & (u == 0))
        def _():
            with jax.named_scope('wait_rail'):
                arrive(k_strip, own)

        @pl.when(first & in_b & split & (u == 2))
        def _():
            with jax.named_scope('wait_rail_last'):
                send_l(l_ref, 7, 7, 8, across, KT, KT).wait_recv()
                lb_copy(7, KT, KT).start()

        @pl.when(first & jnp.logical_not(mine) & (idx == 0))
        def _():
            with jax.named_scope('wait_peer'):
                @pl.when(in_a)
                def _():
                    la_copy(i).wait_recv()

                @pl.when(jnp.logical_not(in_a))
                def _():
                    wait_peer(k_strip)

        @pl.when(first & in_b & split & (u == 3))
        def _():
            lb_copy(7, KT, KT).wait_recv()

        @pl.when(is_a & late & (i == 4) & (n == 0) & (u == 0))
        def _():
            with jax.named_scope('relay'):
                for j in range(3):
                    send_c(j)[0].wait_recv()
                    relay(j).start()

        @pl.when(((is_a & late & (i == 4)) | (is_c & in_a & (i == 0)) | (is_d & in_b & (i == 2))) & (u == 0))
        def _():
            with jax.named_scope('wait_b'):
                send_b(n, n, along).wait_recv()

        for j in range(2):
            @pl.when(in_c & (i == 2 * j) & (n == 0) & (u == 0))
            def _():
                with jax.named_scope('wait_b'):
                    send_b_top(j).wait_recv()

        @pl.when(rest & (tt == 0))
        def _():
            k = acc_of(r, pair, n)
            pltpu.make_async_copy(kept(r, i, n), acc.at[k], psem.at[k]).start()

        use_rem = (is_a & late) | (is_c & in_a) | (is_d & in_b) | in_c
        rows = pl.ds(pl.multiple_of(k_strip * S, S), S)
        cols = pl.ds(pl.multiple_of((kt % 2) * KT, KT), KT)
        for take, ref in (
            (in_a & mine, l_ref),
            (in_a & jnp.logical_not(mine), lap),
            (jnp.logical_not(in_a) & mine, lbr),
            (jnp.logical_not(in_a) & jnp.logical_not(mine), lbp),
        ):
            @pl.when(take)
            def _():
                pltpu.make_async_copy(ref.at[rows, cols], lt.at[slot], lsem.at[slot]).start()
        depth = pl.ds(pl.multiple_of(kt * KT, KT), KT)
        ncols = pl.ds(pl.multiple_of(n * NT, NT), NT)
        for take, ref in ((use_rem, brem), (jnp.logical_not(use_rem), b_ref)):
            @pl.when(take)
            def _():
                pltpu.make_async_copy(ref.at[depth, ncols], bt.at[slot], bsem.at[slot]).start()

    def finish(r, n):
        late, part, _, i, _, _, _, _, _ = run_of(r)
        head = is_d & (i == 2) & jnp.logical_not(part)

        @pl.when(part)
        def _():
            pltpu.make_async_copy(acc.at[0], pst.at[pl.ds(0, S)], osem).wait()

        @pl.when(head)
        def _():
            pltpu.make_async_copy(ot.at[pl.ds(Q, S - Q)], x_ref.at[pl.ds(0, S - Q), pl.ds(0, NT)], osem).wait()

        @pl.when(jnp.logical_not(part | head))
        def _():
            pltpu.make_async_copy(ot, x_ref.at[pl.ds(0, S), pl.ds(0, NT)], osem).wait()

        @pl.when(late & is_b & (i == 2))
        def _():
            send_x_head(n, r - 8).start()

        @pl.when(late & jnp.logical_not(is_b & (i == 2)))
        def _():
            send_x(i, n, jnp.where(is_a, r - 16, r - 8)).start()

    steps = pick(68, 44, 104, 84)
    fetch(jnp.int32(0), jnp.int32(0), 0)

    def step(s, state):
        r, t, waiting, r_old, n_old = state
        late, part, rest, i, n_run, pair, na, nb, nc = run_of(r)
        n, tt = place(n_run, pair, t)
        total = na + nb + nc
        ends = t + 1 == jnp.where(pair, 2 * total, total)
        r_next = jnp.where(ends, r + 1, r)
        t_next = jnp.where(ends, 0, t + 1)
        slot = s % 2
        last = tt + 1 == total
        k = acc_of(r, pair, n)
        late_old = pick(r_old >= 16, r_old >= 8, False, False)

        @pl.when((waiting == 1) & late_old)
        def _():
            finish(r_old, n_old)

        stalls = (is_a & (r_next == 20) & (t_next == 0)) | (is_d & (r_next == 17) & (t_next == 4))

        @pl.when((s + 1 < steps) & jnp.logical_not(stalls))
        def _():
            fetch(r_next, t_next, 1 - slot)

        @pl.when((tt == 0) & rest)
        def _():
            pltpu.make_async_copy(pst.at[pl.ds(0, S)], acc.at[k], psem.at[k]).wait()

        @pl.when((tt == 0) & jnp.logical_not(rest))
        def _():
            acc[k] = jnp.zeros_like(acc[k])

        pltpu.make_async_copy(l_ref.at[pl.ds(0, S), pl.ds(0, KT)], lt.at[slot], lsem.at[slot]).wait()
        pltpu.make_async_copy(b_ref.at[pl.ds(0, KT), pl.ds(0, NT)], bt.at[slot], bsem.at[slot]).wait()
        with jax.named_scope('dot'):
            acc[k] += jnp.dot(lt[slot], bt[slot], preferred_element_type=jnp.float32)

        @pl.when((waiting == 1) & jnp.logical_not(late_old))
        def _():
            finish(r_old, n_old)

        @pl.when(last & part)
        def _():
            pltpu.make_async_copy(acc.at[k], kept(r, i, n), osem).start()

        @pl.when(last & jnp.logical_not(part))
        def _():
            ot[...] = acc[k].astype(ot.dtype)
            rows = pl.ds(pl.multiple_of(i * S, S), S)
            staged = pl.ds(pl.multiple_of(i % 4 * S, S), S)
            cols = pl.ds(pl.multiple_of(n * NT, NT), NT)
            head = is_d & (i == 2)

            @pl.when(late)
            def _():
                pltpu.make_async_copy(ot, xst.at[staged, cols], osem).start()

            @pl.when(head)
            def _():
                pltpu.make_async_copy(
                    ot.at[pl.ds(Q, S - Q)], x_ref.at[pl.ds(2 * S + Q, S - Q), cols], osem).start()

            @pl.when(jnp.logical_not(late | head))
            def _():
                pltpu.make_async_copy(ot, x_ref.at[rows, cols], osem).start()
        @pl.when(stalls)
        def _():
            @pl.when(last)
            def _():
                finish(r, n)
            fetch(r_next, t_next, 1 - slot)
        return r_next, t_next, jnp.where(last & jnp.logical_not(stalls), 1, 0), r, n

    zero = jnp.int32(0)
    state = lax.fori_loop(0, steps, step, (zero, zero, zero, zero, zero))
    finish(state[3], state[4])

    @pl.when(is_a)
    def _():
        for j in range(3):
            relay(j).wait_send()
        for k in range(8):
            send_x(4 + k % 4, k // 4, k).wait_send()

    @pl.when(is_b)
    def _():
        for k in range(8):
            with jax.named_scope('wait_x_in'):
                send_x(4 + k % 4, k // 4, k).wait_recv()
        with jax.named_scope('wait_x_sent'):
            for k in range(6):
                send_tile_b(k).wait_send()

    @pl.when(is_d)
    def _():
        with jax.named_scope('wait_x_in'):
            for k in range(6):
                send_tile_b(k).wait_recv()

    with jax.named_scope('wait_own_sends'):
        own_sends(lambda copy: copy.wait_send())

    @pl.when(jnp.logical_not(is_a))
    def _():
        @pl.when(is_b)
        def _():
            for k in (4, 5, 8):
                lb_copy(k).wait_send()

            @pl.when(c == 0)
            def _():
                for k in (0, 1, 2, 3, 6, 7, 9):
                    lb_copy(k).wait_send()

        @pl.when(is_c)
        def _():
            @pl.when(c == 0)
            def _():
                for k in range(4):
                    lb_copy(k).wait_send()
            for k in range(4, 8):
                lb_copy(k).wait_send()

        @pl.when(is_d)
        def _():
            for k in range(2, 7):
                lb_copy(k).wait_send()
            lb_copy(7, 0, KT).wait_send()
            lb_copy(7, KT, KT).wait_send()


def solution(mesh):
    block_spec = P(('batch', 'row'), 'col')

    def local_product(l_block, b_block):
        rows, half = l_block.shape
        columns = b_block.shape[1]
        l_like = jax.ShapeDtypeStruct((rows, half), l_block.dtype)
        l_more = jax.ShapeDtypeStruct((rows + 2 * S, half), l_block.dtype)
        b_like = jax.ShapeDtypeStruct((rows, columns), b_block.dtype)
        x_like = jax.ShapeDtypeStruct((rows // 2, columns), b_block.dtype)
        part_like = jax.ShapeDtypeStruct((8 * S, NT), jnp.float32)
        dma = pltpu.SemaphoreType.DMA
        out = pl.pallas_call(
            kernel,
            out_shape=[b_like, l_like, l_more, l_more, b_like, x_like, part_like],
            in_specs=[pl.BlockSpec(memory_space=pl.ANY)] * 2,
            out_specs=[pl.BlockSpec(memory_space=pl.ANY)] * 7,
            scratch_shapes=[
                pltpu.VMEM((2, S, KT), l_block.dtype),
                pltpu.VMEM((2, KT, NT), b_block.dtype),
                pltpu.VMEM((2, S, NT), jnp.float32),
                pltpu.VMEM((S, NT), b_block.dtype),
                dma((2,)), dma((2,)), dma, dma((2,)), dma,
                dma((4,)), dma((2,)), dma((11,)), dma((10,)),
                dma((8,)), dma((8,)), dma((10,)), dma((10,)), dma((8,)), dma((8,)),
            ],
            compiler_params=pltpu.CompilerParams(
                collective_id=0, has_side_effects=True, vmem_limit_bytes=48 * 2**20),
            name='triangular_product',
        )(l_block, b_block)
        return out[0]

    return jax.shard_map(local_product, mesh=mesh, in_specs=(block_spec, block_spec),
                         out_specs=block_spec, check_vma=False)
```

```python
import jax
import jax.numpy as jnp
from jax import lax
from jax.experimental import pallas as pl
from jax.experimental.pallas import tpu as pltpu
from jax.sharding import PartitionSpec as P

MESH = pl.DeviceIdType.MESH
S = 896
KT = 1792
NT = 1024
Q = 240


def kernel(l_ref, b_ref, x_ref, lap, lbr, lbp, brem, xst, pst, lt, bt, acc, ot,
           lsem, bsem, osem, psem, zsem, bs, br, ls, lr, ps, pr, qs, qr, xs, xr):
    batch, row, col = lax.axis_index('batch'), lax.axis_index('row'), lax.axis_index('col')
    x, c = col // 2, col % 2
    is_a = (row == 0) & (x == 0)
    is_b = (row == 0) & (x == 1)
    is_c = (row == 1) & (x == 0)
    is_d = (row == 1) & (x == 1)
    half = l_ref.shape[1]
    peer = (batch, row, 2 * x + 1 - c)
    across = (batch, row, 2 * (1 - x) + c)
    along = (batch, 1 - row, col)

    barrier = pltpu.get_barrier_semaphore()
    for device in (peer, across, along):
        pl.semaphore_signal(barrier, inc=1, device_id=device, device_id_type=MESH)
    pl.semaphore_wait(barrier, 3)

    def remote(src, dst, send, recv, device):
        return pltpu.make_async_remote_copy(
            src_ref=src, dst_ref=dst, send_sem=send, recv_sem=recv,
            device_id=device, device_id_type=MESH)

    def strip(i, lo=0, width=None):
        return pl.ds(i * S, S), pl.ds(lo, half if width is None else width)

    def send_l(src, i, k, out, device, lo=0, width=None):
        return remote(src.at[strip(i, lo, width)], lbr.at[strip(k, lo, width)],
                      ls.at[out], lr.at[k if lo == 0 else 8], device)

    def tri_width(i, h):
        return min((i + 1) * S - h * half, half)

    def send_tri(i, h):
        return send_l(l_ref, i, i, i, across, 0, tri_width(i, h))

    def send_b(n, out, device):
        cols = pl.ds(n * NT, NT)
        return remote(b_ref.at[:, cols], brem.at[:, cols], bs.at[out], br.at[n], device)

    def send_b_top(j):
        rows = pl.ds(j * KT, KT)
        return remote(b_ref.at[rows], brem.at[rows], bs.at[j], br.at[j], along)

    def send_rows(src, at, to, rows, k, out, device):
        return remote(src.at[pl.ds(at, rows)], lbr.at[pl.ds(to, rows)], ls.at[out], lr.at[k], device)

    def send_rest():
        return send_rows(l_ref, 2 * S + Q, 2 * S + Q, S - Q, 2, 9, across)

    def send_c(i):
        if i < 2:
            return [send_l(l_ref, i, i, i, along)]
        if i == 2:
            return [send_rows(l_ref, 2 * S, 2 * S, Q, 2, 2, along), send_rest()]
        if i < 7:
            return [send_l(l_ref, i, i, i, across)]
        return [send_l(l_ref, i, i, 7, across, 0, KT), send_l(l_ref, i, i, 8, across, KT, KT)]

    def relay(j):
        if j == 2:
            return send_rows(lbr, 2 * S, 8 * S, Q, 8, 10, across)
        return send_l(lbr, j, 4 + j, 8 + j, across)

    def send_l11_top(j):
        if j == 2:
            return send_rows(l_ref, 2 * S, 9 * S, Q, 9, 10, along)
        return send_l(l_ref, j, 6 + j, 8 + j, along, 0, tri_width(j, 0))

    def la_copy(i):
        rows = pl.ds(i * S, S)
        return remote(l_ref.at[rows], lap.at[rows], ps.at[i], pr.at[i], peer)

    def lb_copy(i, lo=0, width=None):
        at = strip(i, lo, width)
        k = i if lo == 0 else 8
        return remote(lbr.at[at], lbp.at[at], qs.at[k], qr.at[k], peer)

    def send_x(i, n, k):
        cols = pl.ds(pl.multiple_of(n * NT, NT), NT)
        src = pl.ds(pl.multiple_of(i % 4 * S, S), S)
        dst = pl.ds(pl.multiple_of(i * S, S), S)
        target = (batch, jnp.where(is_a, row, 1 - row), jnp.where(is_a, 2 * (1 - x) + c, col))
        return remote(xst.at[src, cols], x_ref.at[dst, cols], xs.at[k], xr.at[k], target)

    def send_x_head(n, k):
        cols = pl.ds(pl.multiple_of(n * NT, NT), NT)
        at = (pl.ds(2 * S, Q), cols)
        return remote(xst.at[at], x_ref.at[at], xs.at[k], xr.at[k], along)

    def send_tile_b(k):
        j, n = k % 3, k // 3
        return send_x_head(n, k) if j == 2 else send_x(j, n, k)

    def each_tri(do):
        for h in (0, 1):
            @pl.when(c == h)
            def _():
                for i in range(4 * h, 8):
                    do(i, h)

    def each_la(do):
        @pl.when(is_c | (is_a & (c == 0)))
        def _():
            for i in range(2):
                do(i)

        @pl.when(is_c | (c == 0))
        def _():
            for i in range(2, 4):
                do(i)
        for i in range(4, 8):
            do(i)

    def own_sends(do):
        @pl.when(is_a)
        def _():
            for n in range(2):
                do(send_b(n, n, along))

            @pl.when(c == 0)
            def _():
                for i in range(4):
                    do(send_tri(i, 0))

        @pl.when(is_b)
        def _():
            for n in range(2):
                do(send_b(n, n, along))
                do(send_b(n, 2 + n, across))

        @pl.when(is_c)
        def _():
            for i in range(8):
                for copy in send_c(i):
                    do(copy)

        @pl.when(is_d)
        def _():
            @pl.when(c == 0)
            def _():
                for j in range(3):
                    do(send_l11_top(j))
            for j in range(2):
                do(send_b_top(j))
            each_tri(lambda i, h: do(send_tri(i, h)))

        @pl.when(jnp.logical_not(is_b))
        def _():
            each_la(lambda i: do(la_copy(i)))

    own_sends(lambda copy: copy.start())

    def zero_corner(k, j):
        @pl.when((is_c & (c == k // 4)) | (is_b & (c == 0) & (k != 4)))
        def _():
            cols = pl.ds((1 if k in (0, 4) or j == 6 else 3) * S, S)
            copy = pltpu.make_async_copy(ot.at[:, pl.ds(0, S)], lbr.at[pl.ds(k * S, S), cols], zsem)
            copy.start()
            copy.wait()

    @pl.when(is_b | is_c)
    def _():
        ot[...] = jnp.zeros_like(ot)
        for k in (0, 2, 4):
            zero_corner(k, k)

        @pl.when(is_c & (c == 1))
        def _():
            copy = pltpu.make_async_copy(
                ot.at[:, pl.ds(0, S)], lbr.at[pl.ds(6 * S, S), pl.ds(3 * S, S)], zsem)
            copy.start()
            copy.wait()

        @pl.when(is_b & (c == 0))
        def _():
            copy = pltpu.make_async_copy(
                ot.at[:, pl.ds(0, S)], lbr.at[pl.ds(6 * S, S), pl.ds(S, S)], zsem)
            copy.start()
            copy.wait()

    def pick(a, b, c_, d):
        return jnp.where(is_a, a, jnp.where(is_b, b, jnp.where(is_c, c_, d)))

    def run_of(r):
        late = pick(r >= 16, r >= 8, False, False)
        part = pick(False, False, (r < 3) | ((r >= 6) & (r < 14) & (r % 2 == 1)), r < 8)
        rest = pick(False, False, (r >= 15) & (r < 22), r >= 12)
        pair = is_d & (r >= 16)
        i_c = jnp.where(r < 3, r, jnp.where(r < 6, r - 3, jnp.where(
            r < 15, r // 2, jnp.where(r < 22, r - 15, 7))))
        n_c = jnp.where(r < 3, 1, jnp.where(r < 6, 0, jnp.where(r < 15, r % 2, 1)))
        i_d = jnp.where(r < 4, 2 + r, jnp.where(r < 8, 4 + r // 2, jnp.where(r < 16, 2 + r % 4, r - 10)))
        n_d = jnp.where(r < 4, 1, jnp.where(r < 8, r % 2, jnp.where(r < 12, 0, jnp.where(r < 16, 1, 0))))
        i = pick(jnp.where(late, 4 + r % 4, r % 8), jnp.where(late, (r - 8) % 3, r % 4), i_c, i_d)
        n = pick(jnp.where(late, (r - 16) // 4, r // 8), jnp.where(late, (r - 8) // 3, r // 4), n_c, n_d)
        tri = i // 2 + 1
        na = pick(tri, 0, jnp.where(part, 0, 4), jnp.where(rest, 0, tri))
        nb = pick(0, jnp.where(late, 4, tri), jnp.where(rest, 0, tri), jnp.where(part, 0, 4))
        nc = jnp.where(is_b & late, 1 + i // 2, 0)
        return late, part, rest, i, n, pair, na, nb, nc

    def kept(r, i, n):
        k = jnp.where(is_c, i, jnp.where(r < 8, r, jnp.where(r < 16, r - 12, 2 * i - 8 + n)))
        return pst.at[pl.ds(pl.multiple_of(k * S, S), S)]

    def acc_of(r, pair, n):
        return jnp.where(pair, n, r % 2)

    def place(n, pair, t):
        return jnp.where(pair, t % 2, n), jnp.where(pair, t // 2, t)

    def arrive(k_dyn, own):
        for k in range(8):
            @pl.when(k_dyn == k)
            def _():
                @pl.when(is_d)
                def _():
                    if k == 2:
                        send_rest().wait_recv()
                    elif k < 7:
                        send_l(l_ref, k, k, k, across).wait_recv()
                    else:
                        send_l(l_ref, k, k, k, across, 0, KT).wait_recv()

                @pl.when(is_c)
                def _():
                    for h in (0, 1):
                        if k >= 4 * h:
                            @pl.when(c == h)
                            def _():
                                send_tri(k, h).wait_recv()

                @pl.when(is_b)
                def _():
                    if k in (4, 5):
                        send_l(l_ref, k, k, k, across).wait_recv()
                    else:
                        @pl.when(c == 0)
                        def _():
                            send_l(l_ref, k, k, k, across, 0, tri_width(k % 6, 0)).wait_recv()

                pass_on(k, own)

        @pl.when(is_b)
        def _():
            for k in (8, 9):
                @pl.when((k_dyn == k) & (own > 0))
                def _():
                    send_rows(l_ref, 0, k * S, Q, k, 0, across).wait_recv()
                    lb_copy(k).start()

    def pass_on(k, own):
                @pl.when(own > 0)
                def _():
                    if k < 7:
                        lb_copy(k).start()
                    else:
                        @pl.when(is_d)
                        def _():
                            lb_copy(k, 0, KT).start()

                        @pl.when(jnp.logical_not(is_d))
                        def _():
                            lb_copy(k).start()

    def wait_peer(k_dyn):
        @pl.when(is_b)
        def _():
            for k in (8, 9):
                @pl.when(k_dyn == k)
                def _():
                    lb_copy(k).wait_recv()

        for k in range(8):
            @pl.when(k_dyn == k)
            def _():
                if k < 7:
                    lb_copy(k).wait_recv()
                else:
                    @pl.when(is_d)
                    def _():
                        lb_copy(k, 0, KT).wait_recv()

                    @pl.when(jnp.logical_not(is_d))
                    def _():
                        lb_copy(k).wait_recv()

    def fetch(r, t, slot):
        late, _, rest, i, n_run, pair, na, nb, nc = run_of(r)
        n, tt = place(n_run, pair, t)
        in_a = tt < na
        in_c = tt >= na + nb
        in_b = jnp.logical_not(in_a) & jnp.logical_not(in_c)
        u = jnp.where(in_a, tt, jnp.where(in_c, tt - na - nb, tt - na))
        nk = jnp.where(in_a, na, jnp.where(in_c, nc, nb))
        full = (is_c & in_a) | (is_d & in_b) | (is_b & late & in_b)
        low = jnp.minimum(nk, 2)
        own = jnp.where(c == 0, low, nk - low)
        mine = (full & (u % 2 == 0)) | (jnp.logical_not(full) & (u < own))
        idx = jnp.where(full, u // 2, jnp.where(mine, u, u - own))
        kt = jnp.where(mine, 2 * c, 2 * (1 - c)) + idx
        k_strip = jnp.where(is_b & late, jnp.where(
            i == 2, jnp.where(in_c, 9, 8), jnp.where(in_c, 6 + i, 4 + i)), i)
        first = pick((n == 0) & jnp.logical_not(late), n == 0,
                     (in_a & (n == 0)) | (jnp.logical_not(in_a) & ((r < 3) | ((r >= 6) & (r < 15) & (r % 2 == 0)))),
                     jnp.where(in_a, (r < 5) | (r == 6), n == 0))
        split = is_d & (i == 7)

        @pl.when(is_a & late & (i == 4) & (n == 0) & (u == 0))
        def _():
            with jax.named_scope('relay'):
                for j in range(3):
                    send_c(j)[0].wait_recv()
                    relay(j).start()

        @pl.when(((is_a & late & (i == 4)) | (is_c & in_a & (i == 0)) | (is_d & in_b & (i == 2))) & (u == 0))
        def _():
            with jax.named_scope('wait_b'):
                send_b(n, n, along).wait_recv()

        for j in range(2):
            @pl.when(in_c & (i == 2 * j) & (n == 0) & (u == 0))
            def _():
                with jax.named_scope('wait_b'):
                    send_b_top(j).wait_recv()

        @pl.when(rest & (tt == 0))
        def _():
            k = acc_of(r, pair, n)
            pltpu.make_async_copy(kept(r, i, n), acc.at[k], psem.at[k]).start()

        use_rem = (is_a & late) | (is_c & in_a) | (is_d & in_b) | in_c
        depth = pl.ds(pl.multiple_of(kt * KT, KT), KT)
        ncols = pl.ds(pl.multiple_of(n * NT, NT), NT)
        for take, ref in ((use_rem, brem), (jnp.logical_not(use_rem), b_ref)):
            @pl.when(take)
            def _():
                pltpu.make_async_copy(ref.at[depth, ncols], bt.at[slot], bsem.at[slot]).start()

        @pl.when(first & jnp.logical_not(in_a) & (u == 0))
        def _():
            with jax.named_scope('wait_rail'):
                arrive(k_strip, own)

        @pl.when(first & in_b & split & (u == 2))
        def _():
            with jax.named_scope('wait_rail_last'):
                send_l(l_ref, 7, 7, 8, across, KT, KT).wait_recv()
                lb_copy(7, KT, KT).start()

        @pl.when(first & jnp.logical_not(mine) & (idx == 0))
        def _():
            with jax.named_scope('wait_peer'):
                @pl.when(in_a)
                def _():
                    la_copy(i).wait_recv()

                @pl.when(jnp.logical_not(in_a))
                def _():
                    wait_peer(k_strip)

        @pl.when(first & in_b & split & (u == 3))
        def _():
            lb_copy(7, KT, KT).wait_recv()

        rows = pl.ds(pl.multiple_of(k_strip * S, S), S)
        cols = pl.ds(pl.multiple_of((kt % 2) * KT, KT), KT)
        for take, ref in (
            (in_a & mine, l_ref),
            (in_a & jnp.logical_not(mine), lap),
            (jnp.logical_not(in_a) & mine, lbr),
            (jnp.logical_not(in_a) & jnp.logical_not(mine), lbp),
        ):
            @pl.when(take)
            def _():
                pltpu.make_async_copy(ref.at[rows, cols], lt.at[slot], lsem.at[slot]).start()

    def finish(r, n):
        late, part, _, i, _, _, _, _, _ = run_of(r)
        head = is_d & (i == 2) & jnp.logical_not(part)

        @pl.when(part)
        def _():
            pltpu.make_async_copy(acc.at[0], pst.at[pl.ds(0, S)], osem).wait()

        @pl.when(head)
        def _():
            pltpu.make_async_copy(ot.at[pl.ds(Q, S - Q)], x_ref.at[pl.ds(0, S - Q), pl.ds(0, NT)], osem).wait()

        @pl.when(jnp.logical_not(part | head))
        def _():
            pltpu.make_async_copy(ot, x_ref.at[pl.ds(0, S), pl.ds(0, NT)], osem).wait()

        @pl.when(late & is_b & (i == 2))
        def _():
            send_x_head(n, r - 8).start()

        @pl.when(late & jnp.logical_not(is_b & (i == 2)))
        def _():
            send_x(i, n, jnp.where(is_a, r - 16, r - 8)).start()

    steps = pick(68, 44, 104, 84)
    fetch(jnp.int32(0), jnp.int32(0), 0)

    def step(s, state):
        r, t, waiting, r_old, n_old = state
        late, part, rest, i, n_run, pair, na, nb, nc = run_of(r)
        n, tt = place(n_run, pair, t)
        total = na + nb + nc
        ends = t + 1 == jnp.where(pair, 2 * total, total)
        r_next = jnp.where(ends, r + 1, r)
        t_next = jnp.where(ends, 0, t + 1)
        slot = s % 2
        last = tt + 1 == total
        k = acc_of(r, pair, n)
        late_old = pick(r_old >= 16, r_old >= 8, False, False)

        @pl.when((waiting == 1) & late_old)
        def _():
            finish(r_old, n_old)

        stalls = (is_a & (r_next == 20) & (t_next == 0)) | (is_d & (r_next == 17) & (t_next == 4))

        @pl.when((s + 1 < steps) & jnp.logical_not(stalls))
        def _():
            fetch(r_next, t_next, 1 - slot)

        @pl.when((tt == 0) & rest)
        def _():
            pltpu.make_async_copy(pst.at[pl.ds(0, S)], acc.at[k], psem.at[k]).wait()

        @pl.when((tt == 0) & jnp.logical_not(rest))
        def _():
            acc[k] = jnp.zeros_like(acc[k])

        pltpu.make_async_copy(l_ref.at[pl.ds(0, S), pl.ds(0, KT)], lt.at[slot], lsem.at[slot]).wait()
        pltpu.make_async_copy(b_ref.at[pl.ds(0, KT), pl.ds(0, NT)], bt.at[slot], bsem.at[slot]).wait()
        with jax.named_scope('dot'):
            acc[k] += jnp.dot(lt[slot], bt[slot], preferred_element_type=jnp.float32)

        @pl.when((waiting == 1) & jnp.logical_not(late_old))
        def _():
            finish(r_old, n_old)

        @pl.when(last & part)
        def _():
            pltpu.make_async_copy(acc.at[k], kept(r, i, n), osem).start()

        @pl.when(last & jnp.logical_not(part))
        def _():
            ot[...] = acc[k].astype(ot.dtype)
            rows = pl.ds(pl.multiple_of(i * S, S), S)
            staged = pl.ds(pl.multiple_of(i % 4 * S, S), S)
            cols = pl.ds(pl.multiple_of(n * NT, NT), NT)
            head = is_d & (i == 2)

            @pl.when(late)
            def _():
                pltpu.make_async_copy(ot, xst.at[staged, cols], osem).start()

            @pl.when(head)
            def _():
                pltpu.make_async_copy(
                    ot.at[pl.ds(Q, S - Q)], x_ref.at[pl.ds(2 * S + Q, S - Q), cols], osem).start()

            @pl.when(jnp.logical_not(late | head))
            def _():
                pltpu.make_async_copy(ot, x_ref.at[rows, cols], osem).start()
        @pl.when(stalls)
        def _():
            @pl.when(last)
            def _():
                finish(r, n)
            fetch(r_next, t_next, 1 - slot)
        return r_next, t_next, jnp.where(last & jnp.logical_not(stalls), 1, 0), r, n

    zero = jnp.int32(0)
    state = lax.fori_loop(0, steps, step, (zero, zero, zero, zero, zero))
    finish(state[3], state[4])

    @pl.when(is_a)
    def _():
        for j in range(3):
            relay(j).wait_send()
        for k in range(8):
            send_x(4 + k % 4, k // 4, k).wait_send()

    @pl.when(is_b)
    def _():
        for k in range(8):
            with jax.named_scope('wait_x_in'):
                send_x(4 + k % 4, k // 4, k).wait_recv()
        with jax.named_scope('wait_x_sent'):
            for k in range(6):
                send_tile_b(k).wait_send()

    @pl.when(is_d)
    def _():
        with jax.named_scope('wait_x_in'):
            for k in range(6):
                send_tile_b(k).wait_recv()

    with jax.named_scope('wait_own_sends'):
        own_sends(lambda copy: copy.wait_send())

    @pl.when(jnp.logical_not(is_a))
    def _():
        @pl.when(is_b)
        def _():
            for k in (4, 5, 8):
                lb_copy(k).wait_send()

            @pl.when(c == 0)
            def _():
                for k in (0, 1, 2, 3, 6, 7, 9):
                    lb_copy(k).wait_send()

        @pl.when(is_c)
        def _():
            @pl.when(c == 0)
            def _():
                for k in range(4):
                    lb_copy(k).wait_send()
            for k in range(4, 8):
                lb_copy(k).wait_send()

        @pl.when(is_d)
        def _():
            for k in range(2, 7):
                lb_copy(k).wait_send()
            lb_copy(7, 0, KT).wait_send()
            lb_copy(7, KT, KT).wait_send()


def solution(mesh):
    block_spec = P(('batch', 'row'), 'col')

    def local_product(l_block, b_block):
        rows, half = l_block.shape
        columns = b_block.shape[1]
        l_like = jax.ShapeDtypeStruct((rows, half), l_block.dtype)
        l_more = jax.ShapeDtypeStruct((rows + 2 * S, half), l_block.dtype)
        b_like = jax.ShapeDtypeStruct((rows, columns), b_block.dtype)
        x_like = jax.ShapeDtypeStruct((rows // 2, columns), b_block.dtype)
        part_like = jax.ShapeDtypeStruct((8 * S, NT), jnp.float32)
        dma = pltpu.SemaphoreType.DMA
        out = pl.pallas_call(
            kernel,
            out_shape=[b_like, l_like, l_more, l_more, b_like, x_like, part_like],
            in_specs=[pl.BlockSpec(memory_space=pl.ANY)] * 2,
            out_specs=[pl.BlockSpec(memory_space=pl.ANY)] * 7,
            scratch_shapes=[
                pltpu.VMEM((2, S, KT), l_block.dtype),
                pltpu.VMEM((2, KT, NT), b_block.dtype),
                pltpu.VMEM((2, S, NT), jnp.float32),
                pltpu.VMEM((S, NT), b_block.dtype),
                dma((2,)), dma((2,)), dma, dma((2,)), dma,
                dma((4,)), dma((2,)), dma((11,)), dma((10,)),
                dma((8,)), dma((8,)), dma((10,)), dma((10,)), dma((8,)), dma((8,)),
            ],
            compiler_params=pltpu.CompilerParams(
                collective_id=0, has_side_effects=True, vmem_limit_bytes=48 * 2**20),
            name='triangular_product',
        )(l_block, b_block)
        return out[0]

    return jax.shard_map(local_product, mesh=mesh, in_specs=(block_spec, block_spec),
                         out_specs=block_spec, check_vma=False)
```
